32 devices in a mesh: dp: 1 (over z), tp: 32 (over x, y, core).
Axes of the slice: x: 4, y: 4, z: 1, core: 2. Of those that a mesh axis runs over, the one named last changes fastest.
The devices are a block of a 4x4x8 slice.
Arguments:
- x: bfloat16 [4, 512, 8192], P('dp')
- gain_a: bfloat16 [8192], replicated
- wq: bfloat16 [8192, 8192], P(None, 'tp')
- wk: bfloat16 [8192, 8192], P(None, 'tp')
- wv: bfloat16 [8192, 8192], P(None, 'tp')
- wo: bfloat16 [8192, 8192], P('tp')
- gain_m: bfloat16 [8192], replicated
- w_gate: bfloat16 [8192, 24576], P(None, 'tp')
- w_up: bfloat16 [8192, 24576], P(None, 'tp')
- w_down: bfloat16 [24576, 8192], P('tp')
Outputs:
- output: bfloat16 [4, 512, 8192], P('dp')
All inputs are finite; a program needn't handle non-finite values.
Results may differ from the reference program's by a relative error of at most 0.017.
Values are sent between devices in bfloat16 or wider.
A program may use at most 768 MiB of HBM per device.

```python
import jax
import jax.numpy as jnp
from jax import lax

SEQUENCES = 4
TOKENS = 512
D = 8192
HEADS = 64
KV_HEADS = 64
HEAD = 128
FF = 24576
THETA = 10000


def setup_inputs(seed: int = 0, part: int = 0) -> dict:
    kx, ka, km, kq, kk, kv, ko, kg, ku, kd = jax.random.split(jax.random.key(seed), 10)

    def weights(key, rows, columns):
        return jax.random.normal(key, (rows, columns), jnp.float32) * rows**-0.5

    drawn = {
        "x": jax.random.normal(jax.random.fold_in(kx, part), (SEQUENCES, TOKENS, D), jnp.float32),
        "gain_a": 1 + 0.1 * jax.random.normal(ka, (D,), jnp.float32),
        "wq": 2 * weights(kq, D, HEADS * HEAD),
        "wk": 2 * weights(kk, D, KV_HEADS * HEAD),
        "wv": 4 * weights(kv, D, KV_HEADS * HEAD),
        "wo": weights(ko, HEADS * HEAD, D),
        "gain_m": 1 + 0.1 * jax.random.normal(km, (D,), jnp.float32),
        "w_gate": weights(kg, D, FF),
        "w_up": weights(ku, D, FF),
        "w_down": 3 * weights(kd, FF, D),
    }
    return {k: v.astype(jnp.bfloat16) for k, v in drawn.items()}


def normed(x, gain):
    wide = x.astype(jnp.float32)
    scale = lax.rsqrt(jnp.mean(wide * wide, -1, keepdims=True) + 1e-6)
    return (wide * scale * gain.astype(jnp.float32)).astype(jnp.bfloat16)


def turned(t, place, theta):
    half = t.shape[-1] // 2
    angle = place.astype(jnp.float32)[:, None] * theta ** (-jnp.arange(half, dtype=jnp.float32) / half)
    cos, sin = jnp.cos(angle)[:, None], jnp.sin(angle)[:, None]
    a, b = t[..., :half].astype(jnp.float32), t[..., half:].astype(jnp.float32)
    return jnp.concatenate([a * cos - b * sin, b * cos + a * sin], -1).astype(jnp.bfloat16)


def matmul(a, w):
    return jnp.dot(a, w, preferred_element_type=jnp.float32).astype(jnp.bfloat16)


def einsum(form, a, b):
    return jnp.einsum(form, a.astype(jnp.float32), b.astype(jnp.float32))


def attention(q, k, v):
    scores = einsum("tgsd,ugd->gstu", q, k) * q.shape[-1] ** -0.5
    token = jnp.arange(q.shape[0])
    scores = jnp.where(token[:, None] >= token, scores, -jnp.inf)
    weights = jax.nn.softmax(scores, -1).astype(jnp.bfloat16)
    return einsum("gstu,ugd->tgsd", weights, v).astype(jnp.bfloat16)


def one(x, gain_a, wq, wk, wv, wo, gain_m, w_gate, w_up, w_down):
    rows = x.shape[0]
    a, place = normed(x, gain_a), jnp.arange(rows)
    k = turned(matmul(a, wk).reshape(rows, -1, HEAD), place, THETA)
    q = turned(matmul(a, wq).reshape(rows, -1, HEAD), place, THETA).reshape(rows, k.shape[1], -1, HEAD)
    v = matmul(a, wv).reshape(rows, -1, HEAD)
    seen = attention(q, k, v).reshape(rows, -1)
    h = (x.astype(jnp.float32) + jnp.dot(seen, wo, preferred_element_type=jnp.float32)).astype(jnp.bfloat16)
    b = normed(h, gain_m)
    gate = jnp.dot(b, w_gate, preferred_element_type=jnp.float32)
    up = jnp.dot(b, w_up, preferred_element_type=jnp.float32)
    hidden = (jax.nn.silu(gate) * up).astype(jnp.bfloat16)
    return (h.astype(jnp.float32) + jnp.dot(hidden, w_down, preferred_element_type=jnp.float32)).astype(jnp.bfloat16)


def reference(x, gain_a, wq, wk, wv, wo, gain_m, w_gate, w_up, w_down):
    return lax.map(lambda sequence: one(sequence, gain_a, wq, wk, wv, wo, gain_m, w_gate, w_up, w_down), x)
```

```python
import functools
import math

import jax
import jax.numpy as jnp
from jax import lax
from jax.experimental import pallas as pl
from jax.experimental.pallas import tpu as pltpu
from jax.sharding import PartitionSpec as P

HEAD = 128
THETA = 10000
MESH = pl.DeviceIdType.MESH
BIG = 63 * 2**20
F32 = jnp.float32
HERE, AHEAD, FAR, BEHIND = RING = range(4)
TOP, BOTTOM = HALVES = range(2)
FAR_UP, FAR_DOWN, ONE_UP, ONE_DOWN, SUM_UP, SUM_DOWN = SUMS = range(6)
UPS = (FAR_UP, ONE_UP, SUM_UP)
ANY, VMEM = pl.BlockSpec(memory_space=pl.ANY), pl.BlockSpec(memory_space=pltpu.VMEM)
DMA = pltpu.SemaphoreType.DMA


def _dot(a, b):
    return jnp.dot(a, b, preferred_element_type=F32)


def _at(start, size):
    return pl.ds(pl.multiple_of(start, size), size)


class _Place:
    def __init__(self, side):
        me = lax.axis_index("tp")
        self.c = c = lax.rem(me, 2)
        chip = lax.div(me, 2)
        x, y = lax.div(chip, side), lax.rem(chip, side)
        self.p, self.t = x * (1 - c) + y * c, y * (1 - c) + x * c
        self.sp, self.st = 2 * (side * (1 - c) + c), 2 * (1 - c + side * c)
        self.side, self.sib = side, me + 1 - 2 * c
        self.right, self.left, self.up, self.down = (self.dev(*d) for d in ((AHEAD, HERE), (BEHIND, HERE), (HERE, AHEAD), (HERE, BEHIND)))
        self.near = [self.right, self.left, self.up, self.down]

    def turn(self, a, n):
        return lax.rem(a + n, self.side)

    def dev(self, dp, dt):
        return self.turn(self.p, dp) * self.sp + self.turn(self.t, dt) * self.st + self.c

    def cross(self, dt, dp):
        return self.turn(self.t, dt) * self.st + self.turn(self.p, dp) * self.sp + 1 - self.c


def _greet(devices):
    barrier = pltpu.get_barrier_semaphore()
    for d in devices:
        pl.semaphore_signal(barrier, inc=1, device_id={"tp": d}, device_id_type=MESH)
    pl.semaphore_wait(barrier, len(devices))


class _Mail:
    def __init__(self, sems):
        self.sems, self.sent = sems, []

    def go(self, src, dst, to):
        n = len(self.sent)
        copy = pltpu.make_async_remote_copy(src_ref=src, dst_ref=dst, send_sem=self.sems.at[TOP, n], recv_sem=self.sems.at[BOTTOM, n],
                                            device_id={"tp": to}, device_id_type=MESH)
        copy.start()
        self.sent.append(copy)
        return n

    def got(self, n):
        self.sent[n].wait_recv()

    def end(self):
        for copy in self.sent:
            copy.wait_send()


class _Local:
    def __init__(self, sems):
        self.sems, self.count = sems, 0

    def go(self, src, dst):
        copy = pltpu.make_async_copy(src, dst, self.sems.at[self.count])
        self.count += 1
        copy.start()
        return copy


class _Sum:
    def __init__(self, mail, out, into, up, down):
        self.mail, self.out, self.into, self.up, self.down = mail, out, into, up, down
        self.sent = {}

    def go(self, n):
        self.sent[n] = self.mail.go(self.out.at[n], self.into.at[n], self.up if n in UPS else self.down)

    def put(self, n, value):
        self.out[n] = value.astype(self.out.dtype)
        self.go(n)

    def got(self, n):
        self.mail.got(self.sent[n])
        return self.into[n].astype(F32)

    def begin(self, product, mid):
        out, half, low = self.out, mid.shape[1], self.out.dtype

        def far(here, a):
            out[FAR_UP, :, here] = a[:half].astype(low)
            out[FAR_DOWN, :, here] = a[half:].astype(low)

        def ahead(here, a):
            mid[TOP, :, here] = a[:half]
            out[ONE_UP, :, here] = a[half:].astype(low)

        def behind(here, a):
            out[ONE_DOWN, :, here] = a[:half].astype(low)
            mid[BOTTOM, :, here] = a[half:]

        for d, keep, goes in ((FAR, far, (FAR_UP, FAR_DOWN)), (AHEAD, ahead, (ONE_UP,)), (BEHIND, behind, (ONE_DOWN,))):
            product(d, keep)
            for n in goes:
                self.go(n)

    def middle(self, mid):
        self.put(SUM_UP, mid[TOP] + self.got(FAR_UP))
        self.put(SUM_DOWN, mid[BOTTOM] + self.got(FAR_DOWN))

    def end(self, top, bottom):
        return top + self.got(SUM_UP) + self.got(ONE_DOWN), bottom + self.got(ONE_UP) + self.got(SUM_DOWN)


def _norm(raw, gain, put, rows, few):
    lax.fori_loop(0, rows // few, lambda n, _: _norm_some(raw, gain, put, n, few), None)


def _norm_some(raw, gain, put, n, few):
    d, lanes = raw.shape[1], 128
    here = _at(n * few, few)
    total = jnp.zeros((few, lanes), F32)
    for k in range(0, d, lanes):
        v = raw[here, k : k + lanes].astype(F32)
        total = total + v * v
    scale = lax.rsqrt(jnp.sum(total, -1, keepdims=True) / d + 1e-6)
    for k in range(0, d, lanes):
        v = raw[here, k : k + lanes].astype(F32)
        put(here, slice(k, k + lanes), (v * scale * gain[:, k : k + lanes].astype(F32)).astype(raw.dtype))


def _heads(side, x, gain, cos, sin, wq, wk, wv, wo, wd, seen, spread, wd_sib, xs, b, w, acc, sems, xsem, local):
    at = _Place(side)
    batch, rows, d = x.shape
    piece, k = spread.shape[1], wo.shape[0]
    low = x.dtype

    def fetch(i):
        slot = lax.rem(i, 2)
        return pltpu.make_async_copy(x.at[i], xs.at[slot], xsem.at[slot])

    here = _Local(local)
    fetch(0).start()
    loads = [here.go(m, w.at[i]) for i, m in enumerate((wq, wk, wv))]
    away = (AHEAD, FAR, BEHIND)
    _greet([at.dev(n, HERE) for n in away] + [at.cross(n, HERE) for n in away] + [at.cross(HERE, n) for n in away] + [at.sib])
    mail = _Mail(sems)
    moves = [mail.go(wo.at[:, _at(at.turn((at.p, at.t)[j], n) * piece, piece)], spread.at[pl.ds((2 * n + j) * k, k), :],
                     (at.dev, at.cross)[j](n, HERE)) for n in (AHEAD, BEHIND, FAR, HERE) for j in HALVES if n + j]
    moves.append(mail.go(wd, wd_sib, at.sib))

    def norm_to(slot):
        def put(here, cols, value):
            b[slot, here, cols] = value

        return put

    def turned(a):
        a = a.astype(low).astype(F32)
        return (a * cos[...] + pltpu.roll(a, HEAD // 2, 1) * sin[...]).astype(low)

    parts, few = 16, rows // 16
    deep = d // parts
    fetch(0).wait()
    fetch(1).start()
    _norm(xs.at[0], gain, norm_to(0), rows, few)
    for copy in loads:
        copy.wait()

    def one(i, _):
        slot, later = lax.rem(i, 2), lax.rem(i + 1, 2)

        @pl.when(i + 1 < batch)
        def _():
            fetch(i + 1).wait()

        @pl.when(i + 2 < batch)
        def _():
            fetch(i + 2).start()

        acc[...] = jnp.zeros_like(acc)

        def part(n, _):
            cut = _at(n * deep, deep)
            for m in range(3):
                acc[m] += _dot(b[slot, :, cut], w[m, cut, :])
            _norm_some(xs.at[later], gain, norm_to(later), n, few)

        lax.fori_loop(0, parts, part, None)
        half = rows // 2
        for n in range(k // HEAD):
            head = slice(n * HEAD, (n + 1) * HEAD)
            q, key, v = turned(acc[0, :, head]), turned(acc[1, :, head]), acc[2, :, head].astype(low)
            for first in (0, half):
                keys = first + half
                score = lax.dot_general(q[first:keys], key[:keys], (((1,), (1,)), ((), ())), preferred_element_type=F32) * HEAD**-0.5
                ok = lax.broadcasted_iota(jnp.int32, score.shape, 0) + first >= lax.broadcasted_iota(jnp.int32, score.shape, 1)
                score = jnp.where(ok, score, -jnp.inf)
                e = jnp.exp(score - jnp.max(score, -1, keepdims=True))
                weights = (e * (1 / jnp.sum(e, -1, keepdims=True))).astype(low)
                seen[_at(i * rows + first, half), head] = _dot(weights, v[:keys]).astype(low)

    lax.fori_loop(0, batch, one, None)
    for n in moves:
        mail.got(n)
    mail.end()


def heads(side, x, gain, cos, sin, wq, wk, wv, wo, wd):
    batch, rows, d = x.shape
    k, low = wo.shape[0], x.dtype
    return pl.pallas_call(
        functools.partial(_heads, side),
        out_shape=[jax.ShapeDtypeStruct((batch * rows, k), low), jax.ShapeDtypeStruct((2 * side * k, d // side), low),
                   jax.ShapeDtypeStruct(wd.shape, low)],
        in_specs=[ANY] + [VMEM] * 3 + [ANY] * 5,
        out_specs=[VMEM, ANY, ANY],
        scratch_shapes=[pltpu.VMEM((2, rows, d), low), pltpu.VMEM((2, rows, d), low), pltpu.VMEM((3, d, k), low),
                        pltpu.VMEM((3, rows, k), F32), DMA((2, 2 * side)), DMA((2,)), DMA((3,))],
        compiler_params=pltpu.CompilerParams(collective_id=4, has_side_effects=True, vmem_limit_bytes=BIG),
        name="heads",
    )(x, gain, cos, sin, wq, wk, wv, wo, wd)


def _first_sum(side, seen, x, wo, spread, h_ref, g, w, mid, out, into, sems, local):
    at = _Place(side)
    count, rows, k = g.shape
    block, cols = h_ref.shape
    here = _Local(local)
    mine = here.go(seen.at[_at(at.c * rows, rows), :], g.at[0])
    rest = pl.ds(k, (count - 1) * k)
    loads = [here.go(wo.at[:, _at(at.p * cols, cols)], w.at[pl.ds(0, k), :]), here.go(spread.at[rest, :], w.at[rest, :])]
    xs = here.go(x.at[_at(at.c * rows + at.t * block, block), _at(at.p * cols, cols)], h_ref)
    _greet(at.near + [at.sib])
    mail = _Mail(sems)
    own, twin, left_own, left_twin, far_own, far_twin, right_own, right_twin = (g.at[n] for n in range(count))
    first = mail.go(seen.at[_at((1 - at.c) * rows, rows), :], twin, at.sib)
    mine.wait()
    a = mail.go(own, left_own, at.right)
    mail.got(first)
    b = mail.go(twin, right_twin, at.left)
    last = [mail.go(own, right_own, at.left), mail.go(twin, left_twin, at.right)]
    mail.got(a)
    last.append(mail.go(left_own, far_own, at.right))
    mail.got(b)
    last.append(mail.go(right_twin, far_twin, at.left))
    for copy in loads:
        copy.wait()
    for n in last:
        mail.got(n)
    wide = cols // 4

    def product(d, put):
        here = _at(at.turn(at.t, d) * block, block)

        def tile(n, _):
            cut = _at(n * wide, wide)
            put(cut, sum(_dot(g[i, here, :], w[pl.ds(i * k, k), cut]) for i in range(count)))

        lax.fori_loop(0, cols // wide, tile, None)

    ring = _Sum(mail, out, into, at.up, at.down)
    ring.begin(product, mid)
    ring.middle(mid)
    half = block // 2

    def keep(cut, a):
        mid[TOP, :, cut] = a[:half]
        mid[BOTTOM, :, cut] = a[half:]

    product(HERE, keep)
    xs.wait()
    top, bottom = ring.end(mid[TOP], mid[BOTTOM])
    h_ref[:half] = (h_ref[:half].astype(F32) + top).astype(h_ref.dtype)
    h_ref[half:] = (h_ref[half:].astype(F32) + bottom).astype(h_ref.dtype)
    mail.end()


def first_sum(side, seen, x, wo, spread):
    tokens, k = seen.shape
    cols, low = spread.shape[1], seen.dtype
    rows = tokens // 2
    block = rows // side
    halves = (len(SUMS), block // 2, cols)
    return pl.pallas_call(
        functools.partial(_first_sum, side),
        out_shape=jax.ShapeDtypeStruct((block, cols), low),
        in_specs=[ANY] * 4,
        out_specs=VMEM,
        scratch_shapes=[pltpu.VMEM((2 * side, rows, k), low), pltpu.VMEM(spread.shape, low), pltpu.VMEM((2, *halves[1:]), F32),
                        pltpu.VMEM(halves, low), pltpu.VMEM(halves, low), DMA((2, 13)), DMA((4,))],
        compiler_params=pltpu.CompilerParams(collective_id=0, has_side_effects=True, vmem_limit_bytes=BIG),
        name="first_sum",
    )(seen, x, wo, spread)


def _gated(side, h, gain, wg, wu, own_hid, sib_hid, every, raw, lhs, hid, wgs, wus, sems, local):
    at = _Place(side)
    block, piece = h.shape
    half, quarter = block // 2, block // 4
    rows = side * block
    ff, low = wgs.shape[1], h.dtype
    here = _Local(local)
    loads = [here.go(wg, wgs), here.go(wu, wus)]
    _greet(at.near + [at.sib])
    mail = _Mail(sems)

    def spot(part, dp):
        return raw.at[pl.ds(part * half, half), _at(at.turn(at.p, dp) * piece, piece)]

    first = [mail.go(h.at[pl.ds(part * half, half), :], spot(part, HERE), to)
             for part, to in ((TOP, at.right), (BOTTOM, at.left), (BOTTOM, at.right), (TOP, at.left))]
    raw[:, _at(at.p * piece, piece)] = h[...]
    for n, part, back, to in zip(first, HALVES, (BEHIND, AHEAD), (at.right, at.left)):
        mail.got(n)
        first.append(mail.go(spot(part, back), spot(part, back), to))
    for n in first[2:]:
        mail.got(n)

    def put(here, cols, value):
        lhs[0, here, cols] = value

    _norm(raw, gain, put, block, 32)

    def ours(d, start, size):
        return every.at[_at(at.c * rows + at.turn(at.t, d) * block + start, size), :]

    def theirs(d, start, size):
        return every.at[_at((1 - at.c) * rows + at.turn(at.p, d) * block + start, size), :]

    on = {}

    def hand(src, stretch):
        on[stretch] = mail.go(src, theirs_there(stretch), at.sib)

    def theirs_there(stretch):
        return ours(*stretch)

    ends = [(HERE, 0, half), (HERE, half, half)]
    b = [lhs.at[0, pl.ds(start, size), :] for _, start, size in ends]
    come = {}
    for parts, to, back in ((HALVES, at.up, BEHIND), (HALVES[::-1], at.down, AHEAD)):
        for part in parts:
            come[back, part] = mail.go(b[part], ours(*ends[part]), to)
    for part in HALVES:
        hand(b[part], ends[part])
    whole = [(HERE, ends[TOP], ends[BOTTOM])]
    steps = [[(BEHIND, 0, half), (AHEAD, half, half)], [(BEHIND, half, half), (AHEAD, 0, half)],
             [(FAR, 0, quarter), (FAR, half, quarter)], [(FAR, quarter, quarter), (FAR, half + quarter, quarter)]]
    back = {stretch: come[stretch[0], min(stretch[1], 1)] for pair in steps[:2] for stretch in pair}
    stores, sums, done = [], [], 0

    def forward(pair):
        for stretch, to, start in zip(pair, (at.up, at.down), (0, half)):
            mail.got(back[stretch])
            if pair is steps[0]:
                for s in (start, start + quarter):
                    ref = ours(stretch[0], s, quarter)
                    back[FAR, s, quarter] = mail.go(ref, ref, to)
            hand(ours(*stretch), stretch)

    def multiply(slot, off, pair, done):
        size = pair[0][2]
        count = 4 * size

        def tile(n, _):
            cut = _at(n * 256, 256)
            gate, up = (_dot(lhs[slot, off : off + count, :], w[:, cut]) for w in (wgs, wus))
            hid[done : done + count, cut] = (jax.nn.silu(gate) * up).astype(low)

        lax.fori_loop(0, ff // 256, tile, None)
        for j, (d, start, size) in enumerate(pair):
            stores.append(here.go(hid.at[pl.ds(done + j * size, size), :], own_hid.at[_at(at.turn(at.t, d) * block + start, size), :]))
            sums.append(mail.go(hid.at[pl.ds(done + (2 + j) * size, size), :], sib_hid.at[_at(at.turn(at.p, d) * block + start, size), :], at.sib))
        return done + count

    for slot, off, pair in ((0, 0, ends), (1, 0, steps[0]), (2, 0, steps[1]), (1, 0, steps[2]), (1, block, steps[3])):
        got = []
        size = pair[0][2]
        if pair is not ends:
            forward(pair)
            got += [here.go(ours(*stretch), lhs.at[slot, pl.ds(off + j * size, size), :]) for j, stretch in enumerate(pair)]
        for j, stretch in enumerate(pair):
            mail.got(on[stretch])
            got.append(here.go(theirs(*stretch), lhs.at[slot, pl.ds(off + (2 + j) * size, size), :]))
        for copy in got + loads:
            copy.wait()
        loads = []
        done = multiply(slot, off, pair, done)
    for copy in stores:
        copy.wait()
    for n in sums:
        mail.got(n)
    mail.end()


def gated(side, h, gain, wg, wu):
    block = h.shape[0]
    d, ff = wg.shape
    rows, low = side * block, h.dtype
    return pl.pallas_call(
        functools.partial(_gated, side),
        out_shape=[jax.ShapeDtypeStruct((rows, ff), low)] * 2 + [jax.ShapeDtypeStruct((2 * rows, d), low)],
        in_specs=[VMEM, VMEM, ANY, ANY],
        out_specs=[ANY] * 3,
        scratch_shapes=[pltpu.VMEM((block, d), low), pltpu.VMEM((3, 2 * block, d), low), pltpu.VMEM((2 * rows, ff), low),
                        pltpu.VMEM((d, ff), low), pltpu.VMEM((d, ff), low), DMA((2, 34)), DMA((32,))],
        compiler_params=pltpu.CompilerParams(collective_id=1, has_side_effects=True, vmem_limit_bytes=BIG),
        name="gated",
    )(h, gain, wg, wu)[:2]


def _second_sum(side, h, a_own, a_sib, w_own, w_sib, y_ref, lhs, w, mid, own, out, into, pout, pinto, sems, near, wsem):
    at = _Place(side)
    block, cols = h.shape
    half, low = block // 2, h.dtype
    here = _Local(near)
    loads = [here.go(a, lhs.at[i]) for i, a in enumerate((a_own, a_sib))]
    order = (FAR, AHEAD, BEHIND, HERE)

    def weights(i):
        cut = _at(at.turn(at.p, order[i]) * cols, cols)
        return [pltpu.make_async_copy(m.at[:, cut], w.at[i % 2, j], wsem.at[i, j]) for j, m in enumerate((w_own, w_sib))]

    for i in HALVES:
        for copy in weights(i):
            copy.start()
    _greet(at.near)
    mail = _Mail(sems)
    wide = cols // 4
    rings = [_Sum(mail, out.at[i], into.at[i], at.up, at.down) for i in RING]
    last = _Sum(mail, pout, pinto, at.right, at.left)

    def compute(i, loads):
        for copy in loads + weights(i):
            copy.wait()

        def product(d, put):
            here = _at(at.turn(at.t, d) * block, block)

            def tile(n, _):
                cut = _at(n * wide, wide)
                put(cut, sum(_dot(lhs[j, here, :], w[i % 2, j, :, cut]) for j in HALVES))

            lax.fori_loop(0, cols // wide, tile, None)

        def keep(cut, a):
            own[i % 3, :, cut] = a

        rings[i].begin(product, mid.at[i % 2])
        product(HERE, keep)
        if i + 2 < side:
            for copy in weights(i + 2):
                copy.start()

    def on(i):
        rings[i].middle(mid.at[i % 2])

    def close(i):
        top, bottom = rings[i].end(own[i % 3, :half], own[i % 3, half:])
        if order[i] == FAR:
            last.put(FAR_UP, top)
            last.put(FAR_DOWN, bottom)
        if order[i] == AHEAD:
            last.put(ONE_UP, bottom)
            last.put(SUM_UP, top + last.got(FAR_UP))
        if order[i] == BEHIND:
            last.put(ONE_DOWN, top)
            last.put(SUM_DOWN, bottom + last.got(FAR_DOWN))
        if order[i] == HERE:
            top, bottom = last.end(top, bottom)
            y_ref[:half] = (h[:half].astype(F32) + top).astype(low)
            y_ref[half:] = (h[half:].astype(F32) + bottom).astype(low)

    a, b, c, d = RING
    compute(a, loads)
    on(a)
    compute(b, [])
    on(b)
    compute(c, [])
    close(a)
    on(c)
    compute(d, [])
    on(d)
    close(b)
    close(c)
    close(d)
    mail.end()


def second_sum(side, h, a_own, a_sib, w_own, w_sib):
    block, cols = h.shape
    rows, ff = a_own.shape
    low = h.dtype
    halves = (len(SUMS), block // 2, cols)
    return pl.pallas_call(
        functools.partial(_second_sum, side),
        out_shape=jax.ShapeDtypeStruct((block, cols), low),
        in_specs=[VMEM] + [ANY] * 4,
        out_specs=VMEM,
        scratch_shapes=[pltpu.VMEM((2, rows, ff), low), pltpu.VMEM((2, 2, ff, cols), low), pltpu.VMEM((2, 2, *halves[1:]), F32),
                        pltpu.VMEM((3, block, cols), F32), pltpu.VMEM((side, *halves), low), pltpu.VMEM((side, *halves), low),
                        pltpu.VMEM(halves, low), pltpu.VMEM(halves, low), DMA((2, 30)), DMA((2,)), DMA((side, 2))],
        compiler_params=pltpu.CompilerParams(collective_id=2, has_side_effects=True, vmem_limit_bytes=BIG),
        name="second_sum",
    )(h, a_own, a_sib, w_own, w_sib)


def _gather(side, s, o, sems, local):
    at = _Place(side)
    block, piece = s.shape
    half = block // 2
    rows = side * block

    def ours(d, part, dq):
        return o.at[_at(at.c * rows + at.turn(at.t, d) * block + part * half, half), _at(at.turn(at.p, dq) * piece, piece)]

    mine = [s.at[pl.ds(part * half, half), :] for part in HALVES]
    here = _Local(local)
    stores = [here.go(mine[part], ours(HERE, part, HERE)) for part in HALVES]
    _greet(at.near + [at.sib])
    mail = _Mail(sems)
    come, to_sib = {}, []

    def along(part, dq, src):
        for to, back in ((at.up, BEHIND), (at.down, AHEAD)):
            come[back, part, dq] = mail.go(src, ours(HERE, part, dq), to)
        to_sib.append(mail.go(src, ours(HERE, part, dq), at.sib))

    ways = [(TOP, BEHIND, at.right), (BOTTOM, AHEAD, at.left), (BOTTOM, BEHIND, at.right), (TOP, AHEAD, at.left)]
    first = []
    for part, _, to in ways:
        first.append(mail.go(mine[part], ours(HERE, part, HERE), to))
        if len(first) <= len(mine):
            along(part, HERE, mine[part])

    def from_p(i):
        part, dq, to = ways[i]
        mail.got(first[i])
        src = ours(HERE, part, dq)
        if i in HALVES:
            first.append(mail.go(src, src, to))
            ways.append((part, FAR, to))
        along(part, dq, src)

    def from_t(part, dq):
        for back, to, goes in ((BEHIND, at.up, TOP), (AHEAD, at.down, BOTTOM)):
            mail.got(come[back, part, dq])
            src = ours(back, part, dq)
            if part == goes:
                come[FAR, part, dq] = mail.go(src, src, to)
            to_sib.append(mail.go(src, src, at.sib))

    for i in range(3):
        from_p(2 * i)
        from_p(2 * i + 1)
        if i in HALVES:
            from_t(*((TOP, HERE), (TOP, BEHIND))[i])
            from_t(*((BOTTOM, HERE), (BOTTOM, AHEAD))[i])
    units = [(part, dq) for part, dq in ((BOTTOM, BEHIND), (TOP, AHEAD), (TOP, FAR), (BOTTOM, FAR))]
    for unit in units:
        from_t(*unit)
    for unit in [(TOP, HERE), (BOTTOM, HERE), (TOP, BEHIND), (BOTTOM, AHEAD)] + units:
        mail.got(come[FAR, *unit])
        src = ours(FAR, *unit)
        to_sib.append(mail.go(src, src, at.sib))
    for copy in stores:
        copy.wait()
    for n in to_sib:
        mail.got(n)
    mail.end()


def gather(side, s):
    block, piece = s.shape
    return pl.pallas_call(
        functools.partial(_gather, side),
        out_shape=jax.ShapeDtypeStruct((2 * side * block, side * piece), s.dtype),
        in_specs=[VMEM],
        out_specs=ANY,
        scratch_shapes=[DMA((2, 62)), DMA((2,))],
        compiler_params=pltpu.CompilerParams(collective_id=3, has_side_effects=True, vmem_limit_bytes=8 * 2**20),
        name="gather",
    )(s)


def _settle(s, o, sems):
    parts = sems.shape[0]
    rows = s.shape[0] // parts
    here = _Local(sems)
    copies = [here.go(s.at[pl.ds(i * rows, rows), :], o.at[pl.ds(i * rows, rows), :]) for i in range(parts)]
    for copy in copies:
        copy.wait()


def settle(s):
    return pl.pallas_call(
        _settle, out_shape=jax.ShapeDtypeStruct(s.shape, s.dtype), in_specs=[ANY], out_specs=ANY, scratch_shapes=[DMA((8,))],
        compiler_params=pltpu.CompilerParams(vmem_limit_bytes=2**20), name="settle",
    )(s)


def solution(mesh):
    side = math.isqrt(mesh.shape["tp"] // 2)

    def step(x, gain_a, wq, wk, wv, wo, gain_m, w_gate, w_up, w_down):
        batch, rows, d = x.shape
        half = HEAD // 2
        angle = jnp.arange(rows).astype(F32)[:, None] * THETA ** (-jnp.arange(half, dtype=F32) / half)
        cos, sin = jnp.cos(angle), jnp.sin(angle)
        cos, sin = jnp.concatenate([cos, cos], -1), jnp.concatenate([-sin, sin], -1)
        seen, spread, w_other = heads(side, x, gain_a.reshape(1, d), cos, sin, wq, wk, wv, wo, w_down)
        h = first_sum(side, seen, x.reshape(batch * rows, d), wo, spread)
        own, other = gated(side, h, gain_m.reshape(1, d), w_gate, w_up)
        y = second_sum(side, h, own, other, w_down, w_other)
        return settle(gather(side, y)).reshape(x.shape)

    tokens, whole, columns, rows_of = P("dp", None, None), P(None), P(None, "tp"), P("tp", None)
    return jax.shard_map(
        step,
        mesh=mesh,
        in_specs=(tokens, whole, columns, columns, columns, rows_of, whole, columns, columns, rows_of),
        out_specs=tokens,
        check_vma=False,
    )
```

```python
import functools
import math

import jax
import jax.numpy as jnp
from jax import lax
from jax.experimental import pallas as pl
from jax.experimental.pallas import tpu as pltpu
from jax.sharding import PartitionSpec as P

HEAD = 128
THETA = 10000
MESH = pl.DeviceIdType.MESH
BIG = 63 * 2**20
F32 = jnp.float32
HERE, AHEAD, FAR, BEHIND = RING = range(4)
TOP, BOTTOM = HALVES = range(2)
FAR_UP, FAR_DOWN, ONE_UP, ONE_DOWN, SUM_UP, SUM_DOWN = SUMS = range(6)
UPS = (FAR_UP, ONE_UP, SUM_UP)
ANY, VMEM = pl.BlockSpec(memory_space=pl.ANY), pl.BlockSpec(memory_space=pltpu.VMEM)
DMA = pltpu.SemaphoreType.DMA


def _dot(a, b):
    return jnp.dot(a, b, preferred_element_type=F32)


def _at(start, size):
    return pl.ds(pl.multiple_of(start, size), size)


class _Place:
    def __init__(self, side):
        me = lax.axis_index("tp")
        self.c = c = lax.rem(me, 2)
        chip = lax.div(me, 2)
        x, y = lax.div(chip, side), lax.rem(chip, side)
        self.p, self.t = x * (1 - c) + y * c, y * (1 - c) + x * c
        self.sp, self.st = 2 * (side * (1 - c) + c), 2 * (1 - c + side * c)
        self.side, self.sib = side, me + 1 - 2 * c
        self.right, self.left, self.up, self.down = (self.dev(*d) for d in ((AHEAD, HERE), (BEHIND, HERE), (HERE, AHEAD), (HERE, BEHIND)))
        self.near = [self.right, self.left, self.up, self.down]

    def turn(self, a, n):
        return lax.rem(a + n, self.side)

    def dev(self, dp, dt):
        return self.turn(self.p, dp) * self.sp + self.turn(self.t, dt) * self.st + self.c

    def cross(self, dt, dp):
        return self.turn(self.t, dt) * self.st + self.turn(self.p, dp) * self.sp + 1 - self.c


def _greet(devices):
    barrier = pltpu.get_barrier_semaphore()
    for d in devices:
        pl.semaphore_signal(barrier, inc=1, device_id={"tp": d}, device_id_type=MESH)
    pl.semaphore_wait(barrier, len(devices))


class _Mail:
    def __init__(self, sems):
        self.sems, self.sent = sems, []

    def go(self, src, dst, to):
        n = len(self.sent)
        copy = pltpu.make_async_remote_copy(src_ref=src, dst_ref=dst, send_sem=self.sems.at[TOP, n], recv_sem=self.sems.at[BOTTOM, n],
                                            device_id={"tp": to}, device_id_type=MESH)
        copy.start()
        self.sent.append(copy)
        return n

    def got(self, n):
        self.sent[n].wait_recv()

    def end(self):
        for copy in self.sent:
            copy.wait_send()


class _Local:
    def __init__(self, sems):
        self.sems, self.count = sems, 0

    def go(self, src, dst):
        copy = pltpu.make_async_copy(src, dst, self.sems.at[self.count])
        self.count += 1
        copy.start()
        return copy


class _Sum:
    def __init__(self, mail, out, into, up, down):
        self.mail, self.out, self.into, self.up, self.down = mail, out, into, up, down
        self.sent = {}

    def go(self, n):
        self.sent[n] = self.mail.go(self.out.at[n], self.into.at[n], self.up if n in UPS else self.down)

    def put(self, n, value):
        def some(rows):
            self.out[n, rows] = value(rows).astype(self.out.dtype)

        _by_rows(self.out.shape[1], some)
        self.go(n)

    def wait(self, *numbers):
        for n in numbers:
            self.mail.got(self.sent[n])

    def read(self, n, rows):
        return self.into[n, rows].astype(F32)

    def begin(self, product, mid):
        out, half, low = self.out, mid.shape[1], self.out.dtype

        def far(here, a):
            out[FAR_UP, :, here] = a[:half].astype(low)
            out[FAR_DOWN, :, here] = a[half:].astype(low)

        def ahead(here, a):
            mid[TOP, :, here] = a[:half]
            out[ONE_UP, :, here] = a[half:].astype(low)

        def behind(here, a):
            out[ONE_DOWN, :, here] = a[:half].astype(low)
            mid[BOTTOM, :, here] = a[half:]

        for d, keep, goes in ((FAR, far, (FAR_UP, FAR_DOWN)), (AHEAD, ahead, (ONE_UP,)), (BEHIND, behind, (ONE_DOWN,))):
            product(d, keep)
            for n in goes:
                self.go(n)

    def middle(self, mid):
        for n, part, far in ((SUM_UP, TOP, FAR_UP), (SUM_DOWN, BOTTOM, FAR_DOWN)):
            self.wait(far)
            self.put(n, lambda rows: mid[part, rows] + self.read(far, rows))

    def end(self, half, put):
        self.wait(ONE_UP, ONE_DOWN, SUM_UP, SUM_DOWN)
        for part, a, b in ((TOP, SUM_UP, ONE_DOWN), (BOTTOM, ONE_UP, SUM_DOWN)):
            _by_rows(half, lambda rows: put(part, rows, self.read(a, rows) + self.read(b, rows)))


def _by_rows(count, some):
    few = 32
    lax.fori_loop(0, count // few, lambda n, _: some(_at(n * few, few)), None)


def _below(part, half, rows):
    return pl.ds(pl.multiple_of(part * half + rows.start, rows.size), rows.size)


def _norm_some(raw, gain, put, n, few):
    d, lanes = raw.shape[1], 128
    here = _at(n * few, few)
    total = jnp.zeros((few, lanes), F32)
    for k in range(0, d, lanes):
        v = raw[here, k : k + lanes].astype(F32)
        total = total + v * v
    scale = lax.rsqrt(jnp.sum(total, -1, keepdims=True) / d + 1e-6)
    for k in range(0, d, lanes):
        v = raw[here, k : k + lanes].astype(F32)
        put(here, slice(k, k + lanes), (v * scale * gain[:, k : k + lanes]).astype(raw.dtype))


def _heads(side, x, gain, cos, sin, wq, wk, wv, wo, wd, seen, spread, wd_sib, xs, b, w, sems, xsem, local):
    at = _Place(side)
    batch, rows, d = x.shape
    piece, k = spread.shape[1], wo.shape[0]
    low = x.dtype

    def fetch(i):
        slot = lax.rem(i, 2)
        return pltpu.make_async_copy(x.at[i], xs.at[slot], xsem.at[slot])

    here = _Local(local)
    fetch(0).start()
    loads = [here.go(m, w.at[i]) for i, m in enumerate((wq, wk, wv))]
    away = (AHEAD, FAR, BEHIND)
    _greet([at.dev(n, HERE) for n in away] + [at.cross(n, HERE) for n in away] + [at.cross(HERE, n) for n in away] + [at.sib])
    mail = _Mail(sems)
    moves = [mail.go(wo.at[:, _at(at.turn((at.p, at.t)[j], n) * piece, piece)], spread.at[pl.ds((2 * n + j) * k, k), :],
                     (at.dev, at.cross)[j](n, HERE)) for n in (AHEAD, BEHIND, FAR, HERE) for j in HALVES if n + j]
    moves.append(mail.go(wd, wd_sib, at.sib))

    def turned(a):
        a = a.astype(low).astype(F32)
        return (a * cos[...] + pltpu.roll(a, HEAD // 2, 1) * sin[...]).astype(low)

    few, half = 32, rows // 2

    def put(here, cols, value):
        b[here, cols] = value

    def one(i, _):
        slot = lax.rem(i, 2)
        fetch(i).wait()

        @pl.when(i + 1 < batch)
        def _():
            fetch(i + 1).start()

        lax.fori_loop(0, rows // few, lambda n, _: _norm_some(xs.at[slot], gain, put, n, few), None)

        @pl.when(i == 0)
        def _():
            for copy in loads:
                copy.wait()

        qs, keys, vs = (_dot(b[...], w[n]) for n in range(3))
        vs = vs.astype(low)
        for n in range(k // HEAD):
            head = slice(n * HEAD, (n + 1) * HEAD)
            q, key, v = turned(qs[:, head]), turned(keys[:, head]), vs[:, head]
            for first in (0, half):
                end = first + half
                score = lax.dot_general(q[first:end], key[:end], (((1,), (1,)), ((), ())), preferred_element_type=F32) * HEAD**-0.5
                ok = lax.broadcasted_iota(jnp.int32, score.shape, 0) + first >= lax.broadcasted_iota(jnp.int32, score.shape, 1)
                score = jnp.where(ok, score, -jnp.inf)
                e = jnp.exp(score - jnp.max(score, -1, keepdims=True))
                weights = (e * (1 / jnp.sum(e, -1, keepdims=True))).astype(low)
                seen[_at(i * rows + first, half), head] = _dot(weights, v[:end]).astype(low)

    lax.fori_loop(0, batch, one, None)
    for n in moves:
        mail.got(n)
    mail.end()


def heads(side, x, gain, cos, sin, wq, wk, wv, wo, wd):
    batch, rows, d = x.shape
    k, low = wo.shape[0], x.dtype
    return pl.pallas_call(
        functools.partial(_heads, side),
        out_shape=[jax.ShapeDtypeStruct((batch * rows, k), low), jax.ShapeDtypeStruct((2 * side * k, d // side), low),
                   jax.ShapeDtypeStruct(wd.shape, low)],
        in_specs=[ANY] + [VMEM] * 3 + [ANY] * 5,
        out_specs=[VMEM, ANY, ANY],
        scratch_shapes=[pltpu.VMEM((2, rows, d), low), pltpu.VMEM((rows, d), low), pltpu.VMEM((3, d, k), low),
                        DMA((2, 2 * side)), DMA((2,)), DMA((3,))],
        compiler_params=pltpu.CompilerParams(collective_id=4, has_side_effects=True, vmem_limit_bytes=BIG),
        name="heads",
    )(x, gain, cos, sin, wq, wk, wv, wo, wd)


def _first_sum(side, seen, x, wo, spread, h_ref, g, w, mid, out, into, sems, local):
    at = _Place(side)
    count, rows, k = g.shape
    block, cols = h_ref.shape
    here = _Local(local)
    mine = here.go(seen.at[_at(at.c * rows, rows), :], g.at[0])
    rest = pl.ds(k, (count - 1) * k)
    loads = [here.go(wo.at[:, _at(at.p * cols, cols)], w.at[pl.ds(0, k), :]), here.go(spread.at[rest, :], w.at[rest, :])]
    xs = here.go(x.at[_at(at.c * rows + at.t * block, block), _at(at.p * cols, cols)], h_ref)
    _greet(at.near + [at.sib])
    mail = _Mail(sems)
    own, twin, left_own, left_twin, far_own, far_twin, right_own, right_twin = (g.at[n] for n in range(count))
    first = mail.go(seen.at[_at((1 - at.c) * rows, rows), :], twin, at.sib)
    mine.wait()
    a = mail.go(own, left_own, at.right)
    mail.got(first)
    b = mail.go(twin, right_twin, at.left)
    last = [mail.go(own, right_own, at.left), mail.go(twin, left_twin, at.right)]
    mail.got(a)
    last.append(mail.go(left_own, far_own, at.right))
    mail.got(b)
    last.append(mail.go(right_twin, far_twin, at.left))
    for copy in loads:
        copy.wait()
    for n in last:
        mail.got(n)
    wide = cols // 4

    def product(d, put):
        here = _at(at.turn(at.t, d) * block, block)

        def tile(n, _):
            cut = _at(n * wide, wide)
            put(cut, sum(_dot(g[i, here, :], w[pl.ds(i * k, k), cut]) for i in range(count)))

        lax.fori_loop(0, cols // wide, tile, None)

    ring = _Sum(mail, out, into, at.up, at.down)
    ring.begin(product, mid)
    ring.middle(mid)
    half = block // 2

    def keep(cut, a):
        mid[TOP, :, cut] = a[:half]
        mid[BOTTOM, :, cut] = a[half:]

    product(HERE, keep)
    xs.wait()

    def add(part, rows, come):
        there = _below(part, half, rows)
        h_ref[there] = (h_ref[there].astype(F32) + (mid[part, rows] + come)).astype(h_ref.dtype)

    ring.end(half, add)
    mail.end()


def first_sum(side, seen, x, wo, spread):
    tokens, k = seen.shape
    cols, low = spread.shape[1], seen.dtype
    rows = tokens // 2
    block = rows // side
    halves = (len(SUMS), block // 2, cols)
    return pl.pallas_call(
        functools.partial(_first_sum, side),
        out_shape=jax.ShapeDtypeStruct((block, cols), low),
        in_specs=[ANY] * 4,
        out_specs=VMEM,
        scratch_shapes=[pltpu.VMEM((2 * side, rows, k), low), pltpu.VMEM(spread.shape, low), pltpu.VMEM((2, *halves[1:]), F32),
                        pltpu.VMEM(halves, low), pltpu.VMEM(halves, low), DMA((2, 13)), DMA((4,))],
        compiler_params=pltpu.CompilerParams(collective_id=0, has_side_effects=True, vmem_limit_bytes=BIG),
        name="first_sum",
    )(seen, x, wo, spread)


def _gated(side, h, gain, wg, wu, own_hid, sib_hid, every, raw, lhs, hid, wgs, wus, sems, local):
    at = _Place(side)
    block, piece = h.shape
    half, quarter = block // 2, block // 4
    rows = side * block
    ff, low = wgs.shape[1], h.dtype
    here = _Local(local)
    _greet(at.near + [at.sib])
    mail = _Mail(sems)

    def spot(start, dp):
        return raw.at[pl.ds(start, quarter), _at(at.turn(at.p, dp) * piece, piece)]

    raw[:, _at(at.p * piece, piece)] = h[...]
    come, on, firsts, rests = {}, {}, [], []

    def put(here, cols, value):
        lhs[0, here, cols] = value

    def ours(d, start):
        return every.at[_at(at.c * rows + at.turn(at.t, d) * block + start, quarter), :]

    def theirs(d, start):
        return every.at[_at((1 - at.c) * rows + at.turn(at.p, d) * block + start, quarter), :]

    def share(top, bottom):
        firsts.append([mail.go(h.at[pl.ds(start, quarter), :], spot(start, HERE), to)
                       for start, to in ((top, at.right), (bottom, at.left), (bottom, at.right), (top, at.left))])

    def relay(group, sent):
        rest = sent[2:]
        for n, start, back, to in zip(sent, group, (BEHIND, AHEAD), (at.right, at.left)):
            mail.got(n)
            rest.append(mail.go(spot(start, back), spot(start, back), to))
        rests.append(rest)

    def spread(group, rest):
        for n in rest:
            mail.got(n)
        for start in group:
            lax.fori_loop(start // few, (start + quarter) // few, lambda n, _: _norm_some(raw, gain, put, n, few), None)
        b = {start: lhs.at[0, pl.ds(start, quarter), :] for start in group}
        for order, to, back in ((group, at.up, BEHIND), (group[::-1], at.down, AHEAD)):
            for start in order:
                come[back, start] = mail.go(b[start], ours(HERE, start), to)
        for start in group:
            on[HERE, start] = mail.go(b[start], ours(HERE, start), at.sib)

    few = quarter // 2
    groups = ((0, half), (quarter, half + quarter))
    share(*groups[0])
    relay(groups[0], firsts[0])
    share(*groups[1])
    loads = [here.go(wg, wgs), here.go(wu, wus)]
    spread(groups[0], rests[0])
    relay(groups[1], firsts[1])
    spread(groups[1], rests[1])
    stores, sums, done = [], [], 0

    def forward(stretches, goes):
        for i, (d, start) in enumerate(stretches):
            ref = ours(d, start)
            mail.got(come[d, start])
            if goes and i < len(HALVES):
                come[FAR, start] = mail.go(ref, ref, (at.up, at.down)[i])
            on[d, start] = mail.go(ref, ref, at.sib)

    def multiply(slot, stretches, done):
        count = 2 * len(stretches) * quarter

        def tile(n, _):
            cut = _at(n * wide, wide)
            gate, up = (_dot(lhs[slot, :count, :], w[:, cut]) for w in (wgs, wus))
            hid[done : done + count, cut] = (jax.nn.silu(gate) * up).astype(low)

        wide = 256
        lax.fori_loop(0, ff // wide, tile, None)
        for d, start in stretches:
            stores.append(here.go(hid.at[pl.ds(done, quarter), :], own_hid.at[_at(at.turn(at.t, d) * block + start, quarter), :]))
            done += quarter
        for d, start in stretches:
            sums.append(mail.go(hid.at[pl.ds(done, quarter), :], sib_hid.at[_at(at.turn(at.p, d) * block + start, quarter), :], at.sib))
            done += quarter
        return done

    steps = [(0, [(HERE, start) for start in range(0, block, quarter)])]
    for slot, (top, bottom) in zip((1, 2), groups):
        steps.append((slot, [(BEHIND, top), (AHEAD, bottom), (BEHIND, bottom), (AHEAD, top)]))
    steps.append((1, [(FAR, start) for group in groups for start in group]))
    for i, (slot, stretches) in enumerate(steps):
        got, place = [], 0
        if i:
            forward(stretches, i < len(steps) - 1)
        for keep in (ours, theirs):
            for stretch in stretches:
                if keep is theirs:
                    mail.got(on[stretch])
                if i or keep is theirs:
                    got.append(here.go(keep(*stretch), lhs.at[slot, pl.ds(place, quarter), :]))
                place += quarter
        for copy in got + loads:
            copy.wait()
        loads = []
        done = multiply(slot, stretches, done)
    for copy in stores:
        copy.wait()
    for n in sums:
        mail.got(n)
    mail.end()


def gated(side, h, gain, wg, wu):
    block = h.shape[0]
    d, ff = wg.shape
    rows, low = side * block, h.dtype
    return pl.pallas_call(
        functools.partial(_gated, side),
        out_shape=[jax.ShapeDtypeStruct((rows, ff), low)] * 2 + [jax.ShapeDtypeStruct((2 * rows, d), low)],
        in_specs=[VMEM, VMEM, ANY, ANY],
        out_specs=[ANY] * 3,
        scratch_shapes=[pltpu.VMEM((block, d), low), pltpu.VMEM((3, 2 * block, d), low), pltpu.VMEM((2 * rows, ff), low),
                        pltpu.VMEM((d, ff), low), pltpu.VMEM((d, ff), low), DMA((2, 56)), DMA((46,))],
        compiler_params=pltpu.CompilerParams(collective_id=1, has_side_effects=True, vmem_limit_bytes=BIG),
        name="gated",
    )(h, gain, wg, wu)[:2]


def _second_sum(side, h, a_own, a_sib, w_own, w_sib, y_ref, lhs, w, mid, own, out, into, pout, pinto, sems, near, wsem):
    at = _Place(side)
    block, cols = h.shape
    half, low = block // 2, h.dtype
    here = _Local(near)
    loads = [here.go(a, lhs.at[i]) for i, a in enumerate((a_own, a_sib))]
    order = (FAR, AHEAD, BEHIND, HERE)

    def weights(i):
        cut = _at(at.turn(at.p, order[i]) * cols, cols)
        return [pltpu.make_async_copy(m.at[:, cut], w.at[i % 2, j], wsem.at[i, j]) for j, m in enumerate((w_own, w_sib))]

    for i in HALVES:
        for copy in weights(i):
            copy.start()
    _greet(at.near)
    mail = _Mail(sems)
    wide = cols // 8
    rings = [_Sum(mail, out.at[i], into.at[i], at.up, at.down) for i in RING]
    last = _Sum(mail, pout, pinto, at.right, at.left)

    def compute(i, loads):
        for copy in loads + weights(i):
            copy.wait()

        def product(d, put):
            here = _at(at.turn(at.t, d) * block, block)

            def tile(n, _):
                cut = _at(n * wide, wide)
                put(cut, sum(_dot(lhs[j, here, :], w[i % 2, j, :, cut]) for j in HALVES))

            lax.fori_loop(0, cols // wide, tile, None)

        def keep(cut, a):
            own[i % 3, :, cut] = a

        rings[i].begin(product, mid.at[i % 2])
        product(HERE, keep)
        if i + 2 < side:
            for copy in weights(i + 2):
                copy.start()

    def on(i):
        rings[i].middle(mid.at[i % 2])

    def close(i):
        total = own.at[i % 3]

        def add(part, rows, come):
            there = _below(part, half, rows)
            total[there] = total[there] + come

        def share(part):
            return lambda rows: total[_below(part, half, rows)]

        rings[i].end(half, add)
        if order[i] == FAR:
            last.put(FAR_UP, share(TOP))
            last.put(FAR_DOWN, share(BOTTOM))
        for d, one, part, both, rest, far in ((AHEAD, ONE_UP, BOTTOM, SUM_UP, TOP, FAR_UP), (BEHIND, ONE_DOWN, TOP, SUM_DOWN, BOTTOM, FAR_DOWN)):
            if order[i] == d:
                last.put(one, share(part))
                last.wait(far)
                last.put(both, lambda rows: share(rest)(rows) + last.read(far, rows))
        if order[i] == HERE:

            def finish(part, rows, come):
                there = _below(part, half, rows)
                y_ref[there] = (h[there].astype(F32) + (total[there] + come)).astype(low)

            last.end(half, finish)

    a, b, c, d = RING
    compute(a, loads)
    on(a)
    compute(b, [])
    on(b)
    compute(c, [])
    close(a)
    on(c)
    compute(d, [])
    on(d)
    close(b)
    close(c)
    close(d)
    mail.end()


def second_sum(side, h, a_own, a_sib, w_own, w_sib):
    block, cols = h.shape
    rows, ff = a_own.shape
    low = h.dtype
    halves = (len(SUMS), block // 2, cols)
    return pl.pallas_call(
        functools.partial(_second_sum, side),
        out_shape=jax.ShapeDtypeStruct((block, cols), low),
        in_specs=[VMEM] + [ANY] * 4,
        out_specs=VMEM,
        scratch_shapes=[pltpu.VMEM((2, rows, ff), low), pltpu.VMEM((2, 2, ff, cols), low), pltpu.VMEM((2, 2, *halves[1:]), F32),
                        pltpu.VMEM((3, block, cols), F32), pltpu.VMEM((side, *halves), low), pltpu.VMEM((side, *halves), low),
                        pltpu.VMEM(halves, low), pltpu.VMEM(halves, low), DMA((2, 30)), DMA((2,)), DMA((side, 2))],
        compiler_params=pltpu.CompilerParams(collective_id=2, has_side_effects=True, vmem_limit_bytes=BIG),
        name="second_sum",
    )(h, a_own, a_sib, w_own, w_sib)


def _gather(side, s, o, sems, local):
    at = _Place(side)
    block, piece = s.shape
    half = block // 2
    rows = side * block

    def ours(d, part, dq):
        return o.at[_at(at.c * rows + at.turn(at.t, d) * block + part * half, half), _at(at.turn(at.p, dq) * piece, piece)]

    mine = [s.at[pl.ds(part * half, half), :] for part in HALVES]
    here = _Local(local)
    stores = [here.go(mine[part], ours(HERE, part, HERE)) for part in HALVES]
    _greet(at.near + [at.sib])
    mail = _Mail(sems)
    come, to_sib = {}, []

    def along(part, dq, src):
        for to, back in ((at.up, BEHIND), (at.down, AHEAD)):
            come[back, part, dq] = mail.go(src, ours(HERE, part, dq), to)
        to_sib.append(mail.go(src, ours(HERE, part, dq), at.sib))

    ways = [(TOP, BEHIND, at.right), (BOTTOM, AHEAD, at.left), (BOTTOM, BEHIND, at.right), (TOP, AHEAD, at.left)]
    first = []
    for part, _, to in ways:
        first.append(mail.go(mine[part], ours(HERE, part, HERE), to))
        if len(first) <= len(mine):
            along(part, HERE, mine[part])

    def from_p(i):
        part, dq, to = ways[i]
        mail.got(first[i])
        src = ours(HERE, part, dq)
        if i in HALVES:
            first.append(mail.go(src, src, to))
            ways.append((part, FAR, to))
        along(part, dq, src)

    def from_t(part, dq):
        for back, to, goes in ((BEHIND, at.up, TOP), (AHEAD, at.down, BOTTOM)):
            mail.got(come[back, part, dq])
            src = ours(back, part, dq)
            if part == goes:
                come[FAR, part, dq] = mail.go(src, src, to)
            to_sib.append(mail.go(src, src, at.sib))

    for i in range(3):
        from_p(2 * i)
        from_p(2 * i + 1)
        if i in HALVES:
            from_t(*((TOP, HERE), (TOP, BEHIND))[i])
            from_t(*((BOTTOM, HERE), (BOTTOM, AHEAD))[i])
    units = [(part, dq) for part, dq in ((BOTTOM, BEHIND), (TOP, AHEAD), (TOP, FAR), (BOTTOM, FAR))]
    for unit in units:
        from_t(*unit)
    for unit in [(TOP, HERE), (BOTTOM, HERE), (TOP, BEHIND), (BOTTOM, AHEAD)] + units:
        mail.got(come[FAR, *unit])
        src = ours(FAR, *unit)
        to_sib.append(mail.go(src, src, at.sib))
    for copy in stores:
        copy.wait()
    for n in to_sib:
        mail.got(n)
    mail.end()


def gather(side, s):
    block, piece = s.shape
    return pl.pallas_call(
        functools.partial(_gather, side),
        out_shape=jax.ShapeDtypeStruct((2 * side * block, side * piece), s.dtype),
        in_specs=[VMEM],
        out_specs=ANY,
        scratch_shapes=[DMA((2, 62)), DMA((2,))],
        compiler_params=pltpu.CompilerParams(collective_id=3, has_side_effects=True, vmem_limit_bytes=8 * 2**20),
        name="gather",
    )(s)


def _settle(s, o, sems):
    parts = sems.shape[0]
    rows = s.shape[0] // parts
    here = _Local(sems)
    copies = [here.go(s.at[pl.ds(i * rows, rows), :], o.at[pl.ds(i * rows, rows), :]) for i in range(parts)]
    for copy in copies:
        copy.wait()


def settle(s):
    return pl.pallas_call(
        _settle, out_shape=jax.ShapeDtypeStruct(s.shape, s.dtype), in_specs=[ANY], out_specs=ANY, scratch_shapes=[DMA((8,))],
        compiler_params=pltpu.CompilerParams(vmem_limit_bytes=2**20), name="settle",
    )(s)


def solution(mesh):
    side = math.isqrt(mesh.shape["tp"] // 2)

    def step(x, gain_a, wq, wk, wv, wo, gain_m, w_gate, w_up, w_down):
        batch, rows, d = x.shape
        half = HEAD // 2
        angle = jnp.arange(rows).astype(F32)[:, None] * THETA ** (-jnp.arange(half, dtype=F32) / half)
        cos, sin = jnp.cos(angle), jnp.sin(angle)
        cos, sin = jnp.concatenate([cos, cos], -1), jnp.concatenate([-sin, sin], -1)
        flat = x.reshape(batch * rows, d)
        seen, spread, w_other = heads(side, x, gain_a.astype(F32).reshape(1, d), cos, sin, wq, wk, wv, wo, w_down)
        h = first_sum(side, seen, flat, wo, spread)
        own, other = gated(side, h, gain_m.astype(F32).reshape(1, d), w_gate, w_up)
        y = second_sum(side, h, own, other, w_down, w_other)
        return settle(gather(side, y)).reshape(x.shape)

    tokens, whole, columns, rows_of = P("dp", None, None), P(None), P(None, "tp"), P("tp", None)
    return jax.shard_map(
        step,
        mesh=mesh,
        in_specs=(tokens, whole, columns, columns, columns, rows_of, whole, columns, columns, rows_of),
        out_specs=tokens,
        check_vma=False,
    )
```
